32 devices in a mesh: grp: 4 (over y, x), dev: 8 (over z, core).
Axes of the slice: x: 2, y: 2, z: 4, core: 2. Of those that a mesh axis runs over, the one named last changes fastest.
Arguments:
- embeddings: bfloat16 [262144, 256], P(('grp', 'dev'))
- prior_dist: float32 [262144], P(('grp', 'dev')), may hold values from 1 to 3
- seed_ids: int32 [6, 512], replicated, may hold values from 0 to 262143, as said below
Outputs:
- min_dist: float32 [262144], P(('grp', 'dev'))
- group_means: float32 [6, 4], P(None, 'grp')
The draws below stay inside these ranges and needn't reach their ends.
Inputs may be any that keep to these rules, and one draw needn't show every extreme that they name: `seed_ids`: round r's ids all lie in the rows of group r mod 4, that is from (r mod 4) * 65536 to (r mod 4 + 1) * 65536 - 1; ids may repeat.
All inputs are finite; a program needn't handle non-finite values.
Results may differ from the reference program's by a relative error of at most 0.0003.
Values may be sent and summed in bfloat16 or wider, within the bound.
A program may use at most 64 MiB of HBM per device.

```python
import jax
import jax.numpy as jnp
from jax import lax

W = 256
SEEDS = 512
ROUNDS = 6
ROW_DEV = 8192
GROUP_ROWS = 65536
ROWS = 262144
GROUPS = 4


def draw_embeddings(key, part):
    key_rows, key_scale, key_shift, key_center, key_member = jax.random.split(jax.random.fold_in(key, 11), 5)
    cluster_count = 4 * SEEDS
    member = jax.random.randint(key_member, (ROWS,), 0, cluster_count, dtype=jnp.int32)
    centroids = jax.random.normal(key_center, (cluster_count, W), jnp.float32)
    scales = jnp.exp(jax.random.uniform(key_scale, (cluster_count,), jnp.float32, -0.7, 0.7))
    row_scale = jnp.take(scales, member, axis=0)
    row_center = jnp.take(centroids, member, axis=0)
    noise = jax.random.normal(key_rows, (ROWS, W), jnp.float32)
    values = row_scale[:, None] * (row_center + 0.3 * noise)
    return values.astype(jnp.bfloat16)


def draw_seed_ids(key, part):
    owners = jnp.arange(ROUNDS, dtype=jnp.int32) % GROUPS
    within = jax.random.randint(jax.random.fold_in(key, 23), (ROUNDS, SEEDS), 0, GROUP_ROWS, dtype=jnp.int32)
    return (owners[:, None] * GROUP_ROWS + within).astype(jnp.int32)


def steps_of(own_key, extent, cuts, least, top_value):
    factor_of = 1.0
    for position, blocks in cuts:
        steps = jax.random.uniform(jax.random.fold_in(jax.random.fold_in(own_key, 6), position), (blocks,), jnp.float32, least / len(cuts), top_value / len(cuts))
        factor_of = factor_of * jnp.repeat(jnp.exp(steps), extent[position] // blocks).reshape((-1,) + (1,) * (len(extent) - 1 - position))
    return factor_of


def setup_inputs(seed: int = 0) -> dict:
    key_of = jax.random.split(jax.random.key(seed), 4)
    return {
        "embeddings": draw_embeddings(jax.random.fold_in(key_of[3], 71), 0),
        "prior_dist": jnp.clip(1.0 + 2.0 * jax.random.uniform(key_of[1], (ROWS,), jnp.float32) ** steps_of(key_of[1], (ROWS,), ((0, 32),), -0.2, 0.2), 1.0, 3.0),
        "seed_ids": draw_seed_ids(jax.random.fold_in(key_of[3], 71), 0),
    }


def block_nearest(block, block_norms, centers, seed_norms):
    products = jnp.dot(block, centers.T, preferred_element_type=jnp.float32)
    gaps = jnp.maximum(block_norms[:, None] + seed_norms[None, :] - 2.0 * products, 0.0) / float(W)
    return jnp.min(gaps, axis=1)


def reference(embeddings, prior_dist, seed_ids):
    row_norms = jnp.sum(jnp.square(embeddings.astype(jnp.float32)), axis=1)
    block_count = ROWS // ROW_DEV
    blocks = embeddings.reshape(block_count, ROW_DEV, W)
    norm_blocks = row_norms.reshape(block_count, ROW_DEV)
    current = prior_dist
    means = []
    for round_index in range(ROUNDS):
        centers = jnp.take(embeddings, seed_ids[round_index], axis=0)
        seed_norms = jnp.sum(jnp.square(centers.astype(jnp.float32)), axis=1)

        def one_block(pair):
            return block_nearest(pair[0], pair[1], centers, seed_norms)

        nearest = lax.map(one_block, (blocks, norm_blocks)).reshape(ROWS)
        current = jnp.minimum(current, nearest)
        means.append(jnp.sum(current.reshape(GROUPS, GROUP_ROWS), axis=1) / float(GROUP_ROWS))
    return current, jnp.stack(means)
```

```python
import functools

import jax
import jax.numpy as jnp
from jax import lax
from jax.experimental import pallas as pl
from jax.experimental.pallas import tpu as pltpu
from jax.sharding import PartitionSpec as P

MESH = pl.DeviceIdType.MESH
LOAD_CHUNKS = 8
TILE = 256
NT = (((1,), (1,)), ((), ()))


def kernel(
    sizes, ids_hbm, prior_hbm, e_hbm, dist, means,
    ids, prior, e, ef, pick, out_half, own_half, pin, half, zin, cent, snb, near, rn, part, parts,
    ids_sem, prior_sem, load_sem, p_sem, rs_sem, ag_sem, grp_sem, fwd_sem, mean_sem,
):
    groups, devs, rounds, seeds, rows, width, subs = sizes
    chips = devs // 2
    sub = seeds // subs
    half_rows = sub // 2
    slots = (rounds + groups - 1) // groups
    wide = width // 2
    g, d = lax.axis_index("grp"), lax.axis_index("dev")
    c, h = d // 2, d % 2
    partner = c * 2 + (1 - h)
    row_start = (g * devs + d) * rows
    chunk = rows // LOAD_CHUNKS

    def load(i):
        at = pl.ds(i * chunk, chunk)
        return pltpu.make_async_copy(e_hbm.at[at], e.at[at], load_sem.at[i])

    load_ids = pltpu.make_async_copy(ids_hbm, ids, ids_sem)
    load_prior = pltpu.make_async_copy(prior_hbm, prior, prior_sem)
    for i in range(LOAD_CHUNKS):
        load(i).start()
    load_ids.start()
    load_prior.start()

    barrier = pltpu.get_barrier_semaphore()
    for o in range(1, devs):
        pl.semaphore_signal(barrier, inc=1, device_id=(g, (d + o) % devs), device_id_type=MESH)

    def peer(o):
        total, base = 0, 1
        while base < groups:
            total = total + (((g // base) % 2 + (o // base) % 2) % 2) * base
            base *= 2
        return total

    for o in range(1, groups):
        pl.semaphore_signal(barrier, inc=1, device_id=(peer(o), d), device_id_type=MESH)

    with jax.named_scope("loadconv"):
        ef[:, pl.ds(rows, 8), :] = jnp.zeros((2, 8, wide), jnp.float32)
        for i in range(LOAD_CHUNKS):
            load(i).wait()

            @pl.loop(0, chunk // 256)
            def _(t):
                at = pl.ds(pl.multiple_of(i * chunk + t * 256, 256), 256)
                for b in range(2):
                    ef[b, at, :] = e[at, b * wide : (b + 1) * wide].astype(jnp.float32)

        load_ids.wait()

    def gather(k, s, which, dst):
        with jax.named_scope("gather"):
            r = g + groups * k
            first = s * sub + which * half_rows

            @pl.loop(0, half_rows // 32)
            def _(b):
                for q in range(32):
                    i = b * 32 + q
                    offset = ids[r, first + i] - row_start
                    row = jnp.where((offset >= 0) & (offset < rows), offset, rows)
                    for w in range(2):
                        pick[w, pl.ds(i, 1), :] = ef[w, pl.ds(row, 1), :]

            u = k * subs + s
            for w in range(2):
                dst[u, :, w * wide : (w + 1) * wide] = pick[w].astype(jnp.bfloat16)

    def send(src, dst, sem, k, j, device):
        return pltpu.make_async_remote_copy(
            src_ref=src, dst_ref=dst, send_sem=sem.at[0, k, j], recv_sem=sem.at[1, k, j],
            device_id=device, device_id_type=MESH,
        )

    def block(owner, u):
        return cent.at[owner + groups * (u // subs), u % subs]

    def to_partner(u):
        return send(out_half.at[u], pin.at[u], p_sem, u, 0, (g, partner))

    def scatter(u, o):
        target = (c + o) % chips
        return send(half.at[u, target], zin.at[u, o], rs_sem, u, o, (g, target * 2 + h))

    def spread(u, o):
        ref = block(g, u).at[h, c]
        return send(ref, ref, ag_sem, u, o, (g, ((c + o) % chips) * 2 + h))

    def across(u, o, origin=None):
        ref = block(g if origin is None else origin, u).at[h]
        return send(ref, ref, grp_sem, u, o, (peer(o), d))

    def forward(u, o):
        ref = block(peer(o), u).at[h]
        return send(ref, ref, fwd_sem, u, o, (g, partner))

    def if_held(k, o, f):
        if isinstance(k, int) and groups * (k + 1) <= rounds:
            f()
        else:
            pl.when(peer(o) + groups * k < rounds)(f)

    def pair_sum(u):
        with jax.named_scope("pairsum"):
            to_partner(u).wait_recv()
            both = own_half[u] + pin[u]
            half[u] = both.reshape(half.shape[1:])
            for o in range(1, chips):
                scatter(u, o).start()

    def start_slot(k):
        def f():
            for s in range(subs):
                gather(k, s, 1 - h, out_half)
                if k == 0 and s == 0:
                    with jax.named_scope("barrier"):
                        pl.semaphore_wait(barrier, devs - 1 + groups - 1)
                to_partner(k * subs + s).start()
            for s in range(subs):
                gather(k, s, h, own_half)
            for s in range(subs):
                pair_sum(k * subs + s)

        if_held(k, 0, f)

    for k in range(slots):
        start_slot(k)

    ones_row = jnp.ones((8, width), jnp.bfloat16)

    def row_norms(first, last):
        with jax.named_scope("rownorm"):
            for j in range(first, last):
                at = pl.ds(j * TILE, TILE)
                square = jnp.square(ef[0, at, :]) + jnp.square(ef[1, at, :])
                high = square.astype(jnp.bfloat16)
                low = (square - high.astype(jnp.float32)).astype(jnp.bfloat16)
                both = jnp.concatenate([high, low], axis=1)
                total = lax.dot_general(ones_row, both, NT, preferred_element_type=jnp.float32)
                for q in range(TILE // 128):
                    rn[pl.ds(j * (TILE // 128) + q, 1), :] = total[0:1, q * 128 : (q + 1) * 128]

    def reduce_chips(u):
        def f():
            with jax.named_scope("reducechips"):
                total = half[u, c]
                for o in range(1, chips):
                    scatter(u, o).wait_recv()
                    total += zin[u, o]
                block(g, u)[h, c] = total
                for o in range(1, chips):
                    spread(u, o).start()

        if_held(u // subs, 0, f)

    def share(u):
        def f():
            with jax.named_scope("share"):
                for o in range(1, chips):
                    spread(u, o).wait_recv()
                forward(u, 0).start()
                for o in range(1, groups):
                    across(u, o).start()

        if_held(u // subs, 0, f)

    steps = rows // TILE
    cuts = [steps * i // 4 for i in range(5)]
    row_norms(cuts[0], cuts[1])
    reduce_chips(0)
    row_norms(cuts[1], cuts[2])
    for u in range(1, subs):
        reduce_chips(u)
    row_norms(cuts[2], cuts[3])
    for u in range(subs):
        share(u)
    for u in range(subs, slots * subs):
        reduce_chips(u)
    row_norms(cuts[3], cuts[4])

    def compute(r, read, count, first):
        centers = read()
        values = centers.astype(jnp.float32)
        norms = jnp.sum(values * values, axis=1, keepdims=True)
        snb[0:count, :] = jnp.broadcast_to(0.5 * norms, (count, 128))
        for j in range(rows // TILE):
            products = lax.dot_general(
                read(), e[pl.ds(j * TILE, TILE), :], NT, preferred_element_type=jnp.float32
            )
            for q in range(TILE // 128):
                score = products[:, q * 128 : (q + 1) * 128] - snb[0:count, :]
                best = jnp.max(score, axis=0, keepdims=True)
                at = pl.ds(j * (TILE // 128) + q, 1)
                near[r, at, :] = best if first else jnp.maximum(near[r, at, :], best)

    for s in range(subs):
        with jax.named_scope("waitfwd"):
            forward(s, 0).wait_recv()
        with jax.named_scope("computesub"):
            compute(g, lambda: cent[g, s].reshape(sub, width), sub, s == 0)
    for u in range(subs, slots * subs):
        share(u)

    own_items = slots - 1
    items = own_items + slots * (groups - 1)

    def item(i):
        j = i - own_items
        own = i < own_items
        return jnp.where(own, i + 1, j // (groups - 1)), jnp.where(own, 0, j % (groups - 1) + 1)

    def relay(k, o):
        for s in range(subs):
            across(k * subs + s, o, peer(o)).wait_recv()
            forward(k * subs + s, o).start()

    @pl.loop(0, items)
    def _(i):
        k, o = item(i)
        nk, no = item(i + 1)
        r = peer(o) + groups * k

        @pl.when((i + 1 < items) & (no > 0) & (peer(no) + groups * nk < rounds))
        def _():
            with jax.named_scope("relay"):
                relay(nk, no)

        @pl.when(r < rounds)
        def _():
            with jax.named_scope("waitfwd"):
                for s in range(subs):
                    forward(k * subs + s, o).wait_recv()
            with jax.named_scope("compute"):
                compute(r, lambda: cent[r].reshape(seeds, width), seeds, True)

    with jax.named_scope("final"):
        load_prior.wait()
        current = prior[...]
        norms = rn[...]
        sums = []
        for r in range(rounds):
            gap = jnp.maximum(norms - 2.0 * near[r], 0.0) * (1.0 / width)
            current = jnp.minimum(current, gap)
            sums.append(jnp.sum(current, axis=0, keepdims=True))
        if rounds < 8:
            sums.append(jnp.zeros((8 - rounds, 128), jnp.float32))
        part[...] = jnp.concatenate(sums, axis=0)
        dist[...] = current

    def send_part(o):
        return send(part, parts.at[o], mean_sem, 0, o, (g, (d + o) % devs))

    with jax.named_scope("means"):
        for o in range(1, devs):
            send_part(o).start()
        total = part[...]
        for o in range(1, devs):
            send_part(o).wait_recv()
            total += parts[o]
        means[...] = jnp.broadcast_to(
            jnp.sum(total, axis=1, keepdims=True) / float(rows * devs), (8, 128)
        )

    for o in range(1, devs):
        send_part(o).wait_send()
    for k in range(slots):
        def drain(k=k):
            for u in range(k * subs, (k + 1) * subs):
                to_partner(u).wait_send()
                for o in range(1, chips):
                    scatter(u, o).wait_send()
                    spread(u, o).wait_send()
                for o in range(1, groups):
                    across(u, o).wait_send()

        def drain_forward(k, o):
            for u in range(k * subs, (k + 1) * subs):
                forward(u, o).wait_send()

        if_held(k, 0, drain)
        for o in range(groups):
            if_held(k, o, functools.partial(drain_forward, k, o))


def body(embeddings, prior_dist, seed_ids):
    rows, width = embeddings.shape
    rounds, seeds = seed_ids.shape
    groups, devs = lax.axis_size("grp"), lax.axis_size("dev")
    chips = devs // 2
    slots = (rounds + groups - 1) // groups
    subs = 2 if seeds // 4 // chips >= 16 else 1
    units = slots * subs
    half_rows = seeds // subs // 2
    piece = half_rows // chips
    bf16, f32 = jnp.bfloat16, jnp.float32
    vmem = pl.BlockSpec(memory_space=pltpu.VMEM)
    hbm = pl.BlockSpec(memory_space=pl.ANY)
    dist, means = pl.pallas_call(
        functools.partial(kernel, (groups, devs, rounds, seeds, rows, width, subs)),
        out_shape=(
            jax.ShapeDtypeStruct((rows // 128, 128), f32),
            jax.ShapeDtypeStruct((8, 128), f32),
        ),
        in_specs=[hbm, hbm, hbm],
        out_specs=(vmem, vmem),
        scratch_shapes=[
            pltpu.SMEM((rounds, seeds), jnp.int32),
            pltpu.VMEM((rows // 128, 128), f32),
            pltpu.VMEM((rows, width), bf16),
            pltpu.VMEM((2, rows + 8, width // 2), f32),
            pltpu.VMEM((2, half_rows, width // 2), f32),
            pltpu.VMEM((units, half_rows, width), bf16),
            pltpu.VMEM((units, half_rows, width), bf16),
            pltpu.VMEM((units, half_rows, width), bf16),
            pltpu.VMEM((units, chips, piece, width), bf16),
            pltpu.VMEM((units, chips, piece, width), bf16),
            pltpu.VMEM((rounds, subs, 2, chips, piece, width), bf16),
            pltpu.VMEM((seeds, 128), f32),
            pltpu.VMEM((rounds, rows // 128, 128), f32),
            pltpu.VMEM((rows // 128, 128), f32),
            pltpu.VMEM((8, 128), f32),
            pltpu.VMEM((devs, 8, 128), f32),
            pltpu.SemaphoreType.DMA,
            pltpu.SemaphoreType.DMA,
            pltpu.SemaphoreType.DMA((LOAD_CHUNKS,)),
            pltpu.SemaphoreType.DMA((2, units, 1)),
            pltpu.SemaphoreType.DMA((2, units, chips)),
            pltpu.SemaphoreType.DMA((2, units, chips)),
            pltpu.SemaphoreType.DMA((2, units, groups)),
            pltpu.SemaphoreType.DMA((2, units, groups)),
            pltpu.SemaphoreType.DMA((2, 1, devs)),
        ],
        compiler_params=pltpu.CompilerParams(
            collective_id=0, has_side_effects=True, vmem_limit_bytes=56 * 1024 * 1024
        ),
        name="seed_rounds",
    )(seed_ids, prior_dist.reshape(rows // 128, 128), embeddings)
    return dist.reshape(rows), means[:rounds, :1]


def solution(mesh):
    placed = (P(("grp", "dev"), None), P(("grp", "dev")), P())
    return jax.shard_map(
        body,
        mesh=mesh,
        in_specs=placed,
        out_specs=(P(("grp", "dev")), P(None, "grp")),
        check_vma=False,
    )
```

```python
import functools

import jax
import jax.numpy as jnp
from jax import lax
from jax.experimental import pallas as pl
from jax.experimental.pallas import tpu as pltpu
from jax.sharding import PartitionSpec as P

MESH = pl.DeviceIdType.MESH
LOAD_CHUNKS = 8
TILE = 256
NT = (((1,), (1,)), ((), ()))


def kernel(
    sizes, ids_hbm, prior_hbm, e_hbm, dist, means,
    ids, ids_v, prior, e, ef, pick, out_half, own_half, pin, half, zin, cent, snb, near, rn, part, parts,
    ids_sem, rows_sem, prior_sem, load_sem, sent,
    p_sem, rs_sem, ag_sem, grp_sem, fwd_sem, mean_sem,
):
    groups, devs, rounds, seeds, rows, width, subs = sizes
    chips = devs // 2
    sub = seeds // subs
    half_rows = sub // 2
    slots = (rounds + groups - 1) // groups
    wide = width // 2
    g, d = lax.axis_index("grp"), lax.axis_index("dev")
    c, h = d // 2, d % 2
    owners, others = chips // 2, chips - chips // 2
    first_owner = chips // 4
    w = c - first_owner
    owns = (w >= 0) & (w < owners)
    partner = c * 2 + (1 - h)
    row_start = (g * devs + d) * rows
    chunk = rows // LOAD_CHUNKS

    def load(i):
        at = pl.ds(i * chunk, chunk)
        return pltpu.make_async_copy(e_hbm.at[at], e.at[at], load_sem.at[i])

    load_ids = pltpu.make_async_copy(ids_hbm, ids_v, ids_sem)
    set_ids = pltpu.make_async_copy(ids_v, ids, rows_sem)
    load_prior = pltpu.make_async_copy(prior_hbm, prior, prior_sem)
    load_ids.start()
    for i in range(LOAD_CHUNKS):
        load(i).start()
    load_prior.start()

    barrier = pltpu.get_barrier_semaphore()
    for o in range(1, devs):
        pl.semaphore_signal(barrier, inc=1, device_id=(g, (d + o) % devs), device_id_type=MESH)

    def peer(o):
        total, base = 0, 1
        while base < groups:
            total = total + (((g // base) % 2 + (o // base) % 2) % 2) * base
            base *= 2
        return total

    for o in range(1, groups):
        pl.semaphore_signal(barrier, inc=1, device_id=(peer(o), d), device_id_type=MESH)

    with jax.named_scope("loadconv"):
        load_ids.wait()
        offset = ids_v[...] - row_start
        ids_v[...] = jnp.where((offset >= 0) & (offset < rows), offset, rows)
        ef[:, pl.ds(rows, 8), :] = jnp.zeros((2, 8, wide), jnp.float32)

        @pl.loop(0, rounds)
        def _(r):
            near[r] = jnp.full(near.shape[1:], -1e38, jnp.float32)

        set_ids.start()
        for i in range(LOAD_CHUNKS):
            load(i).wait()

            @pl.loop(0, chunk // 256)
            def _(t):
                at = pl.ds(pl.multiple_of(i * chunk + t * 256, 256), 256)
                for b in range(2):
                    ef[b, at, :] = e[at, b * wide : (b + 1) * wide].astype(jnp.float32)

        set_ids.wait()

    def gather(k, s, which, dst):
        with jax.named_scope("gather"):
            r = g + groups * k
            first = s * sub + which * half_rows

            for i in range(half_rows):
                row = ids[r, first + i]
                for part_of in range(2):
                    pick[part_of, i : i + 1, :] = ef[part_of, pl.ds(row, 1), :]
            u = k * subs + s
            for part_of in range(2):
                at = slice(part_of * wide, (part_of + 1) * wide)
                dst[u, :, at] = pick[part_of].astype(jnp.bfloat16)

    PAIR, SCATTER, SPREAD, ACROSS, FORWARD = (n * slots * groups for n in range(5))
    MEAN = 5 * slots * groups

    def send(src, dst, send_sem, recv_sem, device):
        return pltpu.make_async_remote_copy(
            src_ref=src, dst_ref=dst, send_sem=send_sem, recv_sem=recv_sem,
            device_id=device, device_id_type=MESH,
        )

    def sent_sem(kind, u, q=0):
        return sent.at[kind + u // subs * groups + q]

    def wait_sent(kind, k, q, count):
        ref = e.at[pl.ds(0, count)]
        send(ref, ref, sent.at[kind + k * groups + q], mean_sem, (g, partner)).wait_send()

    def block(owner, u, half_index):
        return cent.at[owner + groups * (u // subs), half_index, u % subs]

    def to_partner(u):
        return send(out_half.at[u], pin.at[u], sent_sem(PAIR, u), p_sem.at[u], (g, partner))

    def scatter(u, target, slot):
        device = (g, (first_owner + target) * 2 + h)
        send_sem = sent_sem(SCATTER, u)
        return send(half.at[u, target], zin.at[u, slot], send_sem, rs_sem.at[u], device)

    def scatter_all(u):
        @pl.when(owns)
        def _():
            for o in range(1, owners):
                scatter(u, (w + o) % owners, o).start()

        @pl.when(jnp.logical_not(owns))
        def _():
            v = jnp.where(c < first_owner, c, c - owners)
            for target in range(owners):
                scatter(u, target, owners + v).start()

    def wait_scatter(u):
        ref = zin.at[u, pl.ds(1, chips - 1)]
        send(ref, ref, sent_sem(SCATTER, u), rs_sem.at[u], (g, partner)).wait_recv()

    def spread(u, o, q):
        ref = block(peer(q), u, h).at[w]
        device = (g, ((c + o) % chips) * 2 + h)
        return send(ref, ref, sent_sem(SPREAD, u, q), ag_sem.at[u, q], device)

    def wait_spread(u, q):
        def wait(count):
            ref = block(peer(q), u, h).at[pl.ds(0, count)]
            send(ref, ref, sent_sem(SPREAD, u, q), ag_sem.at[u, q], (g, partner)).wait_recv()

        if owners > 1:
            pl.when(owns)(functools.partial(wait, owners - 1))
        pl.when(jnp.logical_not(owns))(functools.partial(wait, owners))

    def by_piece(k, o, source):
        if k:
            return True
        twice = source + groups < rounds
        if o == 1:
            return jnp.logical_not(twice)
        return twice if o == groups - 1 else False

    def whole(k, o, source):
        piece = by_piece(k, o, source)
        return not piece if isinstance(piece, bool) else jnp.logical_not(piece)

    def only_if(condition, f):
        if condition is True:
            f()
        elif condition is not False:
            pl.when(condition)(f)

    def across(u, o, origin=None):
        ref = block(g if origin is None else origin, u, h)
        return send(ref, ref, sent_sem(ACROSS, u, o), grp_sem.at[u, o], (peer(o), d))

    def across_piece(u, o, origin=None):
        ref = block(g if origin is None else origin, u, h).at[w]
        return send(ref, ref, sent_sem(ACROSS, u, o), grp_sem.at[u, o], (peer(o), d))

    def forward(u, o):
        ref = block(peer(o), u, h)
        recv_sem = fwd_sem.at[u // subs * groups + o]
        return send(ref, ref, sent_sem(FORWARD, u, o), recv_sem, (g, partner))

    def wait_forward(k, o):
        with jax.named_scope("waitfwd"):
            ref = cent.at[peer(o) + groups * k, 1 - h]
            at = k * groups + o
            send(ref, ref, sent.at[FORWARD + at], fwd_sem.at[at], (g, partner)).wait_recv()

    def if_held(k, o, f):
        if groups * (k + 1) <= rounds:
            f()
        else:
            pl.when(peer(o) + groups * k < rounds)(f)

    def pair_sum(u):
        with jax.named_scope("pairsum"):
            to_partner(u).wait_recv()
            both = own_half[u] + pin[u]
            half[u] = both.reshape(half.shape[1:])

    def add_pair(u):
        if_held(u // subs, 0, functools.partial(pair_sum, u))

    def scatter_unit(u):
        if_held(u // subs, 0, lambda: scatter_all(u))

    def gather_out(u):
        def f():
            gather(u // subs, u % subs, 1 - h, out_half)
            if u == 0:
                with jax.named_scope("barrier"):
                    pl.semaphore_wait(barrier, devs - 1 + groups - 1)
            to_partner(u).start()

        if_held(u // subs, 0, f)

    def gather_own(u):
        if_held(u // subs, 0, lambda: gather(u // subs, u % subs, h, own_half))

    ones_row = jnp.ones((8, width), jnp.bfloat16)

    def row_norms(first, last):
        with jax.named_scope("rownorm"):
            for j in range(first, last):
                at = pl.ds(j * TILE, TILE)
                square = jnp.square(ef[0, at, :]) + jnp.square(ef[1, at, :])
                high = square.astype(jnp.bfloat16)
                low = (square - high.astype(jnp.float32)).astype(jnp.bfloat16)
                both = jnp.concatenate([high, low], axis=1)
                total = lax.dot_general(ones_row, both, NT, preferred_element_type=jnp.float32)
                for q in range(TILE // 128):
                    rn[pl.ds(j * (TILE // 128) + q, 1), :] = total[0:1, q * 128 : (q + 1) * 128]

    def reduce_chips(u):
        def f():
            with jax.named_scope("reduce%d" % u):
                wait_scatter(u)
                total = half[u, w]
                for slot in range(1, chips):
                    total += zin[u, slot]
                block(g, u, h)[w] = total
                for o in range(1, groups):
                    only_if(by_piece(u // subs, o, g), lambda: across_piece(u, o).start())
                for o in range(1, chips):
                    spread(u, o, 0).start()

        if_held(u // subs, 0, lambda: pl.when(owns)(f))

    def pass_piece(u, q):
        def f():
            with jax.named_scope("piece%d_%d" % (u, q)):
                across_piece(u, q, peer(q)).wait_recv()
                for o in range(1, chips):
                    spread(u, o, q).start()

        piece = by_piece(u // subs, q, peer(q))
        if_held(u // subs, q, lambda: only_if(piece, lambda: pl.when(owns)(f)))

    def share(u, q=0):
        def f():
            with jax.named_scope("share%d_%d" % (u, q)):
                k = u // subs
                if q:
                    only_if(by_piece(k, q, peer(q)), lambda: wait_spread(u, q))
                    only_if(whole(k, q, peer(q)), lambda: across(u, q, peer(q)).wait_recv())
                else:
                    wait_spread(u, 0)
                forward(u, q).start()
                if q == 0:
                    for o in range(1, groups):
                        only_if(whole(k, o, g), lambda: across(u, o).start())

        if_held(u // subs, q, f)

    steps = rows // TILE
    first_units = range(subs)
    late_units = range(subs, slots * subs)

    def start_units(units, scatter_now):
        gather_out(units[0])
        gather_own(units[0])
        for before, u in zip(units, units[1:]):
            gather_out(u)
            add_pair(before)
            if scatter_now:
                scatter_unit(before)
            gather_own(u)
        add_pair(units[-1])
        if scatter_now:
            scatter_unit(units[-1])

    start_units(first_units, True)
    if slots > 1:
        start_units(late_units, False)
    for u in first_units:
        reduce_chips(u)
    row_norms(0, steps // 2)
    for u in late_units:
        scatter_unit(u)
    row_norms(steps // 2, steps)
    for q in range(1, groups):
        for u in first_units:
            pass_piece(u, q)
    for u in first_units:
        share(u)

    def compute(r, read, count):
        centers = read()
        values = centers.astype(jnp.float32)
        norms = jnp.sum(values * values, axis=1, keepdims=True)
        snb[0:count, :] = jnp.broadcast_to(0.5 * norms, (count, 128))
        for j in range(rows // TILE):
            products = lax.dot_general(
                read(), e[pl.ds(j * TILE, TILE), :], NT, preferred_element_type=jnp.float32
            )
            for q in range(TILE // 128):
                score = products[:, q * 128 : (q + 1) * 128] - snb[0:count, :]
                best = jnp.max(score, axis=0, keepdims=True)
                at = pl.ds(j * (TILE // 128) + q, 1)
                near[r, at, :] = jnp.maximum(near[r, at, :], best)

    def item(i):
        return i // groups, i % groups

    halved = 3
    items = slots * groups

    def before_half(n):
        i, second = n // 2, n % 2
        if not second:
            if i:
                for u in first_units:
                    share(u, i)
            if i == 2:
                for u in late_units:
                    for q in range(1, groups):
                        pass_piece(u, q)
        else:
            if i == 0:
                for u in late_units:
                    reduce_chips(u)
            wait_forward(0, i)
            if i == halved - 1:
                for u in first_units:
                    share(u, halved)

    @pl.loop(0, 2 * halved)
    def _(n):
        for m in range(2 * halved):
            pl.when(n == m)(functools.partial(before_half, m))
        r = peer(n // 2)
        which = (h + n) % 2
        with jax.named_scope("half"):
            compute(r, lambda: cent[r, which].reshape(seeds // 2, width), seeds // 2)

    def before_item(i):
        if i + 1 < items:
            for s in range(subs):
                share((i + 1) // groups * subs + s, (i + 1) % groups)

    @pl.loop(halved, items)
    def _(i):
        k, o = item(i)
        r = peer(o) + groups * k
        for n in range(halved, items):
            pl.when(i == n)(functools.partial(before_item, n))

        @pl.when(r < rounds)
        def _():
            wait_forward(k, o)
            with jax.named_scope("compute"):
                compute(r, lambda: cent[r].reshape(seeds, width), seeds)

    with jax.named_scope("final"):
        load_prior.wait()
        current = prior[...]
        norms = rn[...]
        sums = []
        for r in range(rounds):
            gap = jnp.maximum(norms - 2.0 * near[r], 0.0) * (1.0 / width)
            current = jnp.minimum(current, gap)
            sums.append(jnp.sum(current, axis=0, keepdims=True))
        if rounds < 8:
            sums.append(jnp.zeros((8 - rounds, 128), jnp.float32))
        part[...] = jnp.concatenate(sums, axis=0)
        dist[...] = current

    def send_part(o):
        return send(part, parts.at[o], sent.at[MEAN], mean_sem, (g, (d + o) % devs))

    for o in range(1, devs):
        send_part(o).start()

    piece = half_rows // owners

    def drain(k, q):
        source = peer(q)
        wait_sent(FORWARD, k, q, subs * half_rows)
        if q == 0:
            wait_sent(PAIR, k, 0, subs * half_rows)
            if owners > 1:
                pl.when(owns)(lambda: wait_sent(SCATTER, k, 0, subs * (owners - 1) * piece))
            others_sent = subs * owners * piece
            pl.when(jnp.logical_not(owns))(lambda: wait_sent(SCATTER, k, 0, others_sent))
            for o in range(1, groups):
                only_if(
                    by_piece(k, o, g),
                    lambda: pl.when(owns)(lambda: wait_sent(ACROSS, k, o, subs * piece)),
                )
                only_if(whole(k, o, g), lambda: wait_sent(ACROSS, k, o, subs * half_rows))

        def spread_sent():
            wait_sent(SPREAD, k, q, subs * (chips - 1) * piece)

        only_if(True if q == 0 else by_piece(k, q, source), lambda: pl.when(owns)(spread_sent))

    with jax.named_scope("drain"):
        for k in range(slots):
            for q in range(groups):
                if_held(k, q, functools.partial(drain, k, q))

    with jax.named_scope("means"):
        total = part[...]
        every = parts.at[pl.ds(1, devs - 1)]
        means_in = send(every, every, sent.at[MEAN], mean_sem, (g, partner))
        means_in.wait_recv()
        for o in range(1, devs):
            total += parts[o]
        column = jnp.sum(total, axis=1, keepdims=True) / float(rows * devs)
        at_row = lax.broadcasted_iota(jnp.int32, (8, 128), 0)
        at_lane = lax.broadcasted_iota(jnp.int32, (8, 128), 1)
        line = jnp.sum(jnp.where(at_row == at_lane, column, 0.0), axis=0, keepdims=True)
        means[...] = jnp.broadcast_to(line, (8, 128))

    means_in.wait_send()


def emit(dist_in, means_in, dist, means):
    dist[...] = dist_in[...]
    means[...] = means_in[0:1, 0 : means.shape[1]]


def body(embeddings, prior_dist, seed_ids):
    rows, width = embeddings.shape
    rounds, seeds = seed_ids.shape
    groups, devs = lax.axis_size("grp"), lax.axis_size("dev")
    chips = devs // 2
    slots = (rounds + groups - 1) // groups
    subs = 2 if seeds // 4 // (chips // 2) >= 16 else 1
    units = slots * subs
    half_rows = seeds // subs // 2
    owners, others = chips // 2, chips - chips // 2
    piece = half_rows // owners
    bf16, f32 = jnp.bfloat16, jnp.float32
    vmem = pl.BlockSpec(memory_space=pltpu.VMEM)
    hbm = pl.BlockSpec(memory_space=pltpu.HBM)
    dist, means = pl.pallas_call(
        functools.partial(kernel, (groups, devs, rounds, seeds, rows, width, subs)),
        out_shape=(pltpu.VMEM((rows // 128, 128), f32), pltpu.VMEM((8, 128), f32)),
        in_specs=[hbm, hbm, hbm],
        out_specs=(vmem, vmem),
        scratch_shapes=[
            pltpu.SMEM((rounds, seeds), jnp.int32),
            pltpu.VMEM((rounds, seeds), jnp.int32),
            pltpu.VMEM((rows // 128, 128), f32),
            pltpu.VMEM((rows, width), bf16),
            pltpu.VMEM((2, rows + 8, width // 2), f32),
            pltpu.VMEM((2, half_rows, width // 2), f32),
            pltpu.VMEM((units, half_rows, width), bf16),
            pltpu.VMEM((units, half_rows, width), bf16),
            pltpu.VMEM((units, half_rows, width), bf16),
            pltpu.VMEM((units, owners, piece, width), bf16),
            pltpu.VMEM((units, owners + others, piece, width), bf16),
            pltpu.VMEM((rounds, 2, subs, owners, piece, width), bf16),
            pltpu.VMEM((seeds, 128), f32),
            pltpu.VMEM((rounds, rows // 128, 128), f32),
            pltpu.VMEM((rows // 128, 128), f32),
            pltpu.VMEM((8, 128), f32),
            pltpu.VMEM((devs, 8, 128), f32),
            pltpu.SemaphoreType.DMA,
            pltpu.SemaphoreType.DMA,
            pltpu.SemaphoreType.DMA,
            pltpu.SemaphoreType.DMA((LOAD_CHUNKS,)),
            pltpu.SemaphoreType.DMA((5 * slots * groups + 1,)),
            pltpu.SemaphoreType.DMA((units,)),
            pltpu.SemaphoreType.DMA((units,)),
            pltpu.SemaphoreType.DMA((units, groups)),
            pltpu.SemaphoreType.DMA((units, groups)),
            pltpu.SemaphoreType.DMA((slots * groups,)),
            pltpu.SemaphoreType.DMA,
        ],
        compiler_params=pltpu.CompilerParams(
            collective_id=0, has_side_effects=True, vmem_limit_bytes=56 * 1024 * 1024
        ),
        name="seed_rounds",
    )(seed_ids, prior_dist.reshape(rows // 128, 128), embeddings)
    dist, means = pl.pallas_call(
        emit,
        out_shape=(
            jax.ShapeDtypeStruct((rows // 128, 128), f32),
            jax.ShapeDtypeStruct((1, rounds), f32),
        ),
        in_specs=[vmem, vmem],
        out_specs=(vmem, vmem),
        compiler_params=pltpu.CompilerParams(vmem_limit_bytes=1024 * 1024),
        name="emit",
    )(dist, means)
    return dist.reshape(rows), means.reshape(rounds, 1)


def solution(mesh):
    placed = (P(("grp", "dev"), None), P(("grp", "dev")), P())
    return jax.shard_map(
        body,
        mesh=mesh,
        in_specs=placed,
        out_specs=(P(("grp", "dev")), P(None, "grp")),
        check_vma=False,
    )
```

```python
import functools

import jax
import jax.numpy as jnp
from jax import lax
from jax.experimental import pallas as pl
from jax.experimental.pallas import tpu as pltpu
from jax.sharding import PartitionSpec as P

MESH = pl.DeviceIdType.MESH
LOAD_CHUNKS = 8
TILE = 256
NT = (((1,), (1,)), ((), ()))


def kernel(
    sizes, ids_hbm, prior_hbm, e_hbm, dist, means,
    ids, prior, e, ef, pick, out_half, own_half, pin, half, zin, cent, snb, near, rn, part, parts,
    ids_sem, prior_sem, load_sem, sent,
    p_sem, rs_sem, ag_sem, grp_sem, fwd_sem, mean_sem,
):
    groups, devs, rounds, seeds, rows, width, subs = sizes
    chips = devs // 2
    sub = seeds // subs
    half_rows = sub // 2
    slots = (rounds + groups - 1) // groups
    wide = width // 2
    g, d = lax.axis_index("grp"), lax.axis_index("dev")
    c, h = d // 2, d % 2
    owners, others = chips // 2, chips - chips // 2
    first_owner = chips // 4
    w = c - first_owner
    twice = g + groups < rounds
    once = jnp.logical_not(twice)
    owns = (w >= 0) & (w < owners)
    partner = c * 2 + (1 - h)
    row_start = (g * devs + d) * rows
    chunk = rows // LOAD_CHUNKS

    def load(i):
        at = pl.ds(i * chunk, chunk)
        return pltpu.make_async_copy(e_hbm.at[at], e.at[at], load_sem.at[i])

    load_ids = pltpu.make_async_copy(ids_hbm, ids, ids_sem)
    load_prior = pltpu.make_async_copy(prior_hbm, prior, prior_sem)
    load_ids.start()
    for i in range(LOAD_CHUNKS):
        load(i).start()
    load_prior.start()

    barrier = pltpu.get_barrier_semaphore()
    for o in range(1, devs):
        pl.semaphore_signal(barrier, inc=1, device_id=(g, (d + o) % devs), device_id_type=MESH)

    def peer(o):
        total, base = 0, 1
        while base < groups:
            total = total + (((g // base) % 2 + (o // base) % 2) % 2) * base
            base *= 2
        return total

    for o in range(1, groups):
        pl.semaphore_signal(barrier, inc=1, device_id=(peer(o), d), device_id_type=MESH)

    with jax.named_scope("loadconv"):
        ef[:, pl.ds(rows, 8), :] = jnp.zeros((2, 8, wide), jnp.float32)

        @pl.loop(0, rounds)
        def _(r):
            near[r] = jnp.full(near.shape[1:], -1e38, jnp.float32)

        for i in range(LOAD_CHUNKS):
            load(i).wait()

            @pl.loop(0, chunk // 256)
            def _(t):
                at = pl.ds(pl.multiple_of(i * chunk + t * 256, 256), 256)
                for b in range(2):
                    ef[b, at, :] = e[at, b * wide : (b + 1) * wide].astype(jnp.float32)

        load_ids.wait()

    def gather(k, s, which, dst):
        with jax.named_scope("gather"):
            r = g + groups * k
            first = s * sub + which * half_rows

            for i in range(half_rows):
                row = jnp.minimum((ids[r, first + i] - row_start) & 0x7FFFFFFF, rows)
                for part_of in range(2):
                    pick[part_of, i : i + 1, :] = ef[part_of, pl.ds(row, 1), :]
            u = k * subs + s
            for part_of in range(2):
                at = slice(part_of * wide, (part_of + 1) * wide)
                dst[u, :, at] = pick[part_of].astype(jnp.bfloat16)

    SPREAD, ACROSS, FORWARD = (n * slots * groups for n in range(3))
    PAIR, SCATTER, MEAN = (3 * slots * groups + n * slots for n in range(3))

    def send(src, dst, send_sem, recv_sem, device):
        return pltpu.make_async_remote_copy(
            src_ref=src, dst_ref=dst, send_sem=send_sem, recv_sem=recv_sem,
            device_id=device, device_id_type=MESH,
        )

    def sent_sem(kind, u, q=0):
        return sent.at[kind + u // subs * (groups if kind < PAIR else 1) + q]

    def wait_sent(kind, k, q, count):
        ref = e.at[pl.ds(0, count)]
        send(ref, ref, sent_sem(kind, k * subs, q), mean_sem, (g, partner)).wait_send()

    def block(owner, u, half_index):
        return cent.at[owner + groups * (u // subs), half_index, u % subs]

    def to_partner(u):
        return send(out_half.at[u], pin.at[u], sent_sem(PAIR, u), p_sem.at[u], (g, partner))

    def scatter(u, target, slot):
        device = (g, (first_owner + target) * 2 + h)
        send_sem = sent_sem(SCATTER, u)
        return send(half.at[u, target], zin.at[u, slot], send_sem, rs_sem.at[u], device)

    def scatter_all(u):
        @pl.when(owns)
        def _():
            for o in range(1, owners):
                scatter(u, (w + o) % owners, o).start()

        @pl.when(jnp.logical_not(owns))
        def _():
            v = jnp.where(c < first_owner, c, c - owners)
            for target in range(owners):
                scatter(u, target, owners + v).start()

    def wait_scatter(u):
        ref = zin.at[u, pl.ds(1, chips - 1)]
        send(ref, ref, sent_sem(SCATTER, u), rs_sem.at[u], (g, partner)).wait_recv()

    def spread(u, o, q):
        ref = block(peer(q), u, h).at[w]
        device = (g, ((c + o) % chips) * 2 + h)
        return send(ref, ref, sent_sem(SPREAD, u, q), ag_sem.at[u, q], device)

    def wait_spread(u, q):
        def wait(count):
            ref = block(peer(q), u, h).at[pl.ds(0, count)]
            send(ref, ref, sent_sem(SPREAD, u, q), ag_sem.at[u, q], (g, partner)).wait_recv()

        if owners > 1:
            pl.when(owns)(functools.partial(wait, owners - 1))
        pl.when(jnp.logical_not(owns))(functools.partial(wait, owners))

    def by_piece(k, o, source):
        if k:
            return True
        source_twice = source + groups < rounds
        if o == 1:
            return jnp.logical_not(source_twice)
        return source_twice if o == 3 else False

    def whole(k, o, source):
        piece = by_piece(k, o, source)
        return not piece if isinstance(piece, bool) else jnp.logical_not(piece)

    def only_if(condition, f):
        if condition is True:
            f()
        elif condition is not False:
            pl.when(condition)(f)

    def across(u, o, origin=None):
        ref = block(g if origin is None else origin, u, h)
        return send(ref, ref, sent_sem(ACROSS, u, o), grp_sem.at[u, o], (peer(o), d))

    def across_piece(u, o, origin=None):
        ref = block(g if origin is None else origin, u, h).at[w]
        return send(ref, ref, sent_sem(ACROSS, u, o), grp_sem.at[u, o], (peer(o), d))

    def forward(u, o):
        ref = block(peer(o), u, h)
        recv_sem = fwd_sem.at[u // subs * groups + o]
        return send(ref, ref, sent_sem(FORWARD, u, o), recv_sem, (g, partner))

    def wait_forward(k, o):
        with jax.named_scope("waitfwd"):
            ref = cent.at[peer(o) + groups * k, 1 - h]
            at = k * groups + o
            send(ref, ref, sent.at[FORWARD + at], fwd_sem.at[at], (g, partner)).wait_recv()

    def if_held(k, o, f):
        if groups * (k + 1) <= rounds:
            f()
        else:
            pl.when(peer(o) + groups * k < rounds)(f)

    def pair_sum(u):
        with jax.named_scope("pairsum"):
            to_partner(u).wait_recv()
            both = own_half[u] + pin[u]
            half[u] = both.reshape(half.shape[1:])

    def add_pair(u):
        if_held(u // subs, 0, functools.partial(pair_sum, u))

    def scatter_unit(u):
        if_held(u // subs, 0, lambda: scatter_all(u))

    def gather_out(u):
        def f():
            gather(u // subs, u % subs, 1 - h, out_half)
            if u == 0:
                with jax.named_scope("barrier"):
                    pl.semaphore_wait(barrier, devs - 1 + groups - 1)
            to_partner(u).start()

        if_held(u // subs, 0, f)

    def gather_own(u):
        if_held(u // subs, 0, lambda: gather(u // subs, u % subs, h, own_half))

    ones_row = jnp.ones((8, width), jnp.bfloat16)

    def row_norms(first, last):
        with jax.named_scope("rownorm"):
            for j in range(first, last):
                at = pl.ds(j * TILE, TILE)
                square = jnp.square(ef[0, at, :]) + jnp.square(ef[1, at, :])
                high = square.astype(jnp.bfloat16)
                low = (square - high.astype(jnp.float32)).astype(jnp.bfloat16)
                both = jnp.concatenate([high, low], axis=1)
                total = lax.dot_general(ones_row, both, NT, preferred_element_type=jnp.float32)
                for q in range(TILE // 128):
                    rn[pl.ds(j * (TILE // 128) + q, 1), :] = total[0:1, q * 128 : (q + 1) * 128]

    def reduce_chips(u):
        def f():
            with jax.named_scope("reduce%d" % u):
                wait_scatter(u)
                total = half[u, w]
                for slot in range(1, chips):
                    total += zin[u, slot]
                block(g, u, h)[w] = total
                for o in range(1, groups):
                    only_if(by_piece(u // subs, o, g), lambda: across_piece(u, o).start())
                for o in range(1, chips):
                    spread(u, o, 0).start()

        if_held(u // subs, 0, lambda: pl.when(owns)(f))

    def pass_piece(u, q):
        def f():
            with jax.named_scope("piece%d_%d" % (u, q)):
                across_piece(u, q, peer(q)).wait_recv()
                for o in range(1, chips):
                    spread(u, o, q).start()

        piece = by_piece(u // subs, q, peer(q))
        if_held(u // subs, q, lambda: only_if(piece, lambda: pl.when(owns)(f)))

    def share(u, q=0):
        def f():
            with jax.named_scope("share%d_%d" % (u, q)):
                k = u // subs
                if q:
                    only_if(by_piece(k, q, peer(q)), lambda: wait_spread(u, q))
                    only_if(whole(k, q, peer(q)), lambda: across(u, q, peer(q)).wait_recv())
                else:
                    wait_spread(u, 0)
                forward(u, q).start()
                if u < subs and q == 0:
                    pl.when(twice)(lambda: across(u, 1).start())
                    pl.when(once)(lambda: across(u, 2).start())

        if_held(u // subs, q, f)

    steps = rows // TILE
    first_units = range(subs)
    late_units = range(subs, slots * subs)

    def start_units(units, scatter_now):
        gather_out(units[0])
        gather_own(units[0])
        for before, u in zip(units, units[1:]):
            gather_out(u)
            add_pair(before)
            if scatter_now:
                scatter_unit(before)
            gather_own(u)
        add_pair(units[-1])
        if scatter_now:
            scatter_unit(units[-1])

    start_units(first_units, True)
    if slots > 1:
        start_units(late_units, False)
    for u in first_units:
        reduce_chips(u)
    row_norms(0, steps // 2)
    for u in late_units:
        scatter_unit(u)
    row_norms(steps // 2, steps)
    for q in range(1, groups):
        for u in first_units:
            pass_piece(u, q)
    for u in first_units:
        share(u)

    def compute(r, read, count):
        centers = read()
        values = centers.astype(jnp.float32)
        norms = jnp.sum(values * values, axis=1, keepdims=True)
        snb[0:count, :] = jnp.broadcast_to(0.5 * norms, (count, 128))
        for j in range(rows // TILE):
            products = lax.dot_general(
                read(), e[pl.ds(j * TILE, TILE), :], NT, preferred_element_type=jnp.float32
            )
            for q in range(TILE // 128):
                score = products[:, q * 128 : (q + 1) * 128] - snb[0:count, :]
                best = jnp.max(score, axis=0, keepdims=True)
                at = pl.ds(j * (TILE // 128) + q, 1)
                near[r, at, :] = jnp.maximum(near[r, at, :], best)

    def lag(u_list, q):
        for u in u_list:
            share(u, q)

    def pieces_in(q):
        for u in late_units:
            pass_piece(u, q)

    def late_pieces_out():
        for u in late_units:
            reduce_chips(u)
        for u in first_units:
            across(u, 2).start()

    def diagonal_out():
        for u in first_units:
            across(u, 3).start()

    HALF, REST, FULL = range(3)
    kinds = [HALF, REST, HALF, REST, HALF, REST, FULL, HALF, REST, FULL]
    two = [
        (0, 0, []),
        (0, 0, [late_pieces_out]),
        (0, 2, [lambda: lag(first_units, 2)]),
        (0, 2, []),
        (0, 1, [lambda: lag(first_units, 1), lambda: pieces_in(1)]),
        (0, 1, [lambda: lag(late_units, 0)]),
        (1, 0, []),
        (0, 3, [lambda: lag(first_units, 3)]),
        (0, 3, [lambda: lag(late_units, 1)]),
        (1, 1, []),
    ]
    one = [
        (0, 0, []),
        (0, 0, []),
        (0, 1, [lambda: lag(first_units, 1), diagonal_out]),
        (0, 1, []),
        (0, 3, [lambda: lag(first_units, 3), lambda: pieces_in(2)]),
        (0, 3, [lambda: lag(first_units, 2), lambda: pieces_in(3)]),
        (0, 2, []),
        (1, 2, [lambda: lag(late_units, 2)]),
        (1, 2, [lambda: lag(late_units, 3)]),
        (1, 3, []),
    ]

    def prepare(kind, k, o, actions):
        for action in actions:
            action()
        if kind != HALF:
            wait_forward(k, o)

    for kind, line_two, line_one in zip(kinds, two, one):
        pl.when(twice)(functools.partial(prepare, kind, *line_two))
        pl.when(once)(functools.partial(prepare, kind, *line_one))
        r = jnp.where(
            twice, peer(line_two[1]) + groups * line_two[0], peer(line_one[1]) + groups * line_one[0]
        )
        if kind == FULL:
            with jax.named_scope("compute"):
                compute(r, lambda: cent[r].reshape(seeds, width), seeds)
        else:
            which = h if kind == HALF else 1 - h
            with jax.named_scope("half"):
                compute(r, lambda: cent[r, which].reshape(seeds // 2, width), seeds // 2)

    with jax.named_scope("final"):
        load_prior.wait()
        current = prior[...]
        norms = rn[...]
        sums = []
        for r in range(rounds):
            gap = jnp.maximum(norms - 2.0 * near[r], 0.0) * (1.0 / width)
            current = jnp.minimum(current, gap)
            sums.append(jnp.sum(current, axis=0, keepdims=True))
        if rounds < 8:
            sums.append(jnp.zeros((8 - rounds, 128), jnp.float32))
        part[...] = jnp.concatenate(sums, axis=0)
        dist[...] = current

    def send_part(o):
        return send(part, parts.at[o], sent.at[MEAN], mean_sem, (g, (d + o) % devs))

    for o in range(1, devs):
        send_part(o).start()

    piece = half_rows // owners

    def drain(k, q):
        source = peer(q)
        wait_sent(FORWARD, k, q, subs * half_rows)
        if q == 0:
            wait_sent(PAIR, k, 0, subs * half_rows)
            if owners > 1:
                pl.when(owns)(lambda: wait_sent(SCATTER, k, 0, subs * (owners - 1) * piece))
            others_sent = subs * owners * piece
            pl.when(jnp.logical_not(owns))(lambda: wait_sent(SCATTER, k, 0, others_sent))
            for o in range(1, groups):
                only_if(
                    by_piece(k, o, g),
                    lambda: pl.when(owns)(lambda: wait_sent(ACROSS, k, o, subs * piece)),
                )
                only_if(whole(k, o, g), lambda: wait_sent(ACROSS, k, o, subs * half_rows))

        def spread_sent():
            wait_sent(SPREAD, k, q, subs * (chips - 1) * piece)

        only_if(True if q == 0 else by_piece(k, q, source), lambda: pl.when(owns)(spread_sent))

    with jax.named_scope("drain"):
        for k in range(slots):
            for q in range(groups):
                if_held(k, q, functools.partial(drain, k, q))

    with jax.named_scope("means"):
        total = part[...]
        every = parts.at[pl.ds(1, devs - 1)]
        means_in = send(every, every, sent.at[MEAN], mean_sem, (g, partner))
        means_in.wait_recv()
        for o in range(1, devs):
            total += parts[o]
        column = jnp.sum(total, axis=1, keepdims=True) / float(rows * devs)
        at_row = lax.broadcasted_iota(jnp.int32, (8, 128), 0)
        at_lane = lax.broadcasted_iota(jnp.int32, (8, 128), 1)
        line = jnp.sum(jnp.where(at_row == at_lane, column, 0.0), axis=0, keepdims=True)
        means[...] = jnp.broadcast_to(line, (8, 128))

    means_in.wait_send()


def emit(dist_in, means_in, dist, means):
    dist[...] = dist_in[...]
    means[...] = means_in[0:1, 0 : means.shape[1]]


def body(embeddings, prior_dist, seed_ids):
    rows, width = embeddings.shape
    rounds, seeds = seed_ids.shape
    groups, devs = lax.axis_size("grp"), lax.axis_size("dev")
    chips = devs // 2
    slots = (rounds + groups - 1) // groups
    subs = 2 if seeds // 4 // (chips // 2) >= 16 else 1
    units = slots * subs
    half_rows = seeds // subs // 2
    owners, others = chips // 2, chips - chips // 2
    piece = half_rows // owners
    bf16, f32 = jnp.bfloat16, jnp.float32
    vmem = pl.BlockSpec(memory_space=pltpu.VMEM)
    hbm = pl.BlockSpec(memory_space=pltpu.HBM)
    dist, means = pl.pallas_call(
        functools.partial(kernel, (groups, devs, rounds, seeds, rows, width, subs)),
        out_shape=(pltpu.VMEM((rows // 128, 128), f32), pltpu.VMEM((8, 128), f32)),
        in_specs=[hbm, hbm, hbm],
        out_specs=(vmem, vmem),
        scratch_shapes=[
            pltpu.SMEM((rounds, seeds), jnp.int32),
            pltpu.VMEM((rows // 128, 128), f32),
            pltpu.VMEM((rows, width), bf16),
            pltpu.VMEM((2, rows + 8, width // 2), f32),
            pltpu.VMEM((2, half_rows, width // 2), f32),
            pltpu.VMEM((units, half_rows, width), bf16),
            pltpu.VMEM((units, half_rows, width), bf16),
            pltpu.VMEM((units, half_rows, width), bf16),
            pltpu.VMEM((units, owners, piece, width), bf16),
            pltpu.VMEM((units, owners + others, piece, width), bf16),
            pltpu.VMEM((rounds, 2, subs, owners, piece, width), bf16),
            pltpu.VMEM((seeds, 128), f32),
            pltpu.VMEM((rounds, rows // 128, 128), f32),
            pltpu.VMEM((rows // 128, 128), f32),
            pltpu.VMEM((8, 128), f32),
            pltpu.VMEM((devs, 8, 128), f32),
            pltpu.SemaphoreType.DMA,
            pltpu.SemaphoreType.DMA,
            pltpu.SemaphoreType.DMA((LOAD_CHUNKS,)),
            pltpu.SemaphoreType.DMA((3 * slots * groups + 2 * slots + 1,)),
            pltpu.SemaphoreType.DMA((units,)),
            pltpu.SemaphoreType.DMA((units,)),
            pltpu.SemaphoreType.DMA((units, groups)),
            pltpu.SemaphoreType.DMA((units, groups)),
            pltpu.SemaphoreType.DMA((slots * groups,)),
            pltpu.SemaphoreType.DMA,
        ],
        compiler_params=pltpu.CompilerParams(
            collective_id=0, has_side_effects=True, vmem_limit_bytes=56 * 1024 * 1024
        ),
        name="seed_rounds",
    )(seed_ids, prior_dist.reshape(rows // 128, 128), embeddings)
    dist, means = pl.pallas_call(
        emit,
        out_shape=(
            jax.ShapeDtypeStruct((rows // 128, 128), f32),
            jax.ShapeDtypeStruct((1, rounds), f32),
        ),
        in_specs=[vmem, vmem],
        out_specs=(vmem, vmem),
        compiler_params=pltpu.CompilerParams(vmem_limit_bytes=1024 * 1024),
        name="emit",
    )(dist, means)
    return dist.reshape(rows), means.reshape(rounds, 1)


def solution(mesh):
    placed = (P(("grp", "dev"), None), P(("grp", "dev")), P())
    return jax.shard_map(
        body,
        mesh=mesh,
        in_specs=placed,
        out_specs=(P(("grp", "dev")), P(None, "grp")),
        check_vma=False,
    )
```

```python
import functools

import jax
import jax.numpy as jnp
from jax import lax
from jax.experimental import pallas as pl
from jax.experimental.pallas import tpu as pltpu
from jax.sharding import PartitionSpec as P

MESH = pl.DeviceIdType.MESH
LOAD_CHUNKS = 4
TILE = 256
NT = (((1,), (1,)), ((), ()))


def kernel(
    sizes, ids_hbm, prior_hbm, e_hbm, dist, means,
    ids, prior, e, ef, pick, out_half, own_half, pin, half, zin, cent, snb, near, rn, part, parts,
    ids_sem, prior_sem, load_sem, sent,
    p_sem, rs_sem, ag_sem, grp_sem, fwd_sem, mean_sem,
):
    groups, devs, rounds, seeds, rows, width, subs = sizes
    chips = devs // 2
    sub = seeds // subs
    half_rows = sub // 2
    slots = (rounds + groups - 1) // groups
    wide = width // 2
    g, d = lax.axis_index("grp"), lax.axis_index("dev")
    c, h = d // 2, d % 2
    owners, others = chips // 2, chips - chips // 2
    first_owner = chips // 4
    w = c - first_owner
    twice = g + groups < rounds
    once = jnp.logical_not(twice)
    owns = (w >= 0) & (w < owners)
    partner = c * 2 + (1 - h)
    row_start = (g * devs + d) * rows
    chunk = rows // LOAD_CHUNKS

    def load(i):
        at = pl.ds(i * chunk, chunk)
        return pltpu.make_async_copy(e_hbm.at[at], e.at[at], load_sem.at[i])

    load_ids = pltpu.make_async_copy(ids_hbm, ids, ids_sem)
    load_prior = pltpu.make_async_copy(prior_hbm, prior, prior_sem)
    load_ids.start()
    for i in range(LOAD_CHUNKS):
        load(i).start()
    load_prior.start()

    barrier = pltpu.get_barrier_semaphore()
    for o in range(1, devs):
        pl.semaphore_signal(barrier, inc=1, device_id=(g, (d + o) % devs), device_id_type=MESH)

    def peer(o):
        total, base = 0, 1
        while base < groups:
            total = total + (((g // base) % 2 + (o // base) % 2) % 2) * base
            base *= 2
        return total

    for o in range(1, groups):
        pl.semaphore_signal(barrier, inc=1, device_id=(peer(o), d), device_id_type=MESH)

    with jax.named_scope("loadconv"):
        ef[:, pl.ds(rows, 8), :] = jnp.zeros((2, 8, wide), jnp.float32)

        @pl.loop(0, rounds)
        def _(r):
            near[r] = jnp.full(near.shape[1:], -1e38, jnp.float32)

        for i in range(LOAD_CHUNKS):
            load(i).wait()

            @pl.loop(0, chunk // 256)
            def _(t):
                at = pl.ds(pl.multiple_of(i * chunk + t * 256, 256), 256)
                for b in range(2):
                    ef[b, at, :] = e[at, b * wide : (b + 1) * wide].astype(jnp.float32)

        load_ids.wait()

    def gather(k, s, which, dst):
        with jax.named_scope("gather"):
            r = g + groups * k
            first = s * sub + which * half_rows

            for i in range(half_rows):
                row = jnp.minimum((ids[r, first + i] - row_start) & 0x7FFFFFFF, rows)
                for part_of in range(2):
                    pick[part_of, i : i + 1, :] = ef[part_of, pl.ds(row, 1), :]
            u = k * subs + s
            for part_of in range(2):
                at = slice(part_of * wide, (part_of + 1) * wide)
                dst[u, :, at] = pick[part_of].astype(jnp.bfloat16)

    SPREAD, ACROSS, FORWARD, PAIR, SCATTER, MEAN = range(6)

    def send(src, dst, send_sem, recv_sem, device):
        return pltpu.make_async_remote_copy(
            src_ref=src, dst_ref=dst, send_sem=send_sem, recv_sem=recv_sem,
            device_id=device, device_id_type=MESH,
        )

    def wait_sent(kind, count):
        if count:
            ref = e.at[pl.ds(0, count)]
            send(ref, ref, sent.at[kind], mean_sem, (g, partner)).wait_send()

    def block(owner, u, half_index):
        return cent.at[owner + groups * (u // subs), half_index, u % subs]

    def to_partner(u):
        return send(out_half.at[u], pin.at[u], sent.at[PAIR], p_sem.at[u], (g, partner))

    def scatter(u, target, slot):
        device = (g, (first_owner + target) * 2 + h)
        send_sem = sent.at[SCATTER]
        return send(half.at[u, target], zin.at[u, slot], send_sem, rs_sem.at[u], device)

    def scatter_all(u):
        @pl.when(owns)
        def _():
            for o in range(1, owners):
                scatter(u, (w + o) % owners, o).start()

        @pl.when(jnp.logical_not(owns))
        def _():
            v = jnp.where(c < first_owner, c, c - owners)
            for target in range(owners):
                scatter(u, target, owners + v).start()

    def wait_scatter(u):
        ref = zin.at[u, pl.ds(1, chips - 1)]
        send(ref, ref, sent.at[SCATTER], rs_sem.at[u], (g, partner)).wait_recv()

    def spread(u, o, q):
        ref = block(peer(q), u, h).at[w]
        v = o - owners
        other = v + jnp.where(v < first_owner, 0, owners) if o >= owners else (w + o) % owners + first_owner
        device = (g, other * 2 + h)
        return send(ref, ref, sent.at[SPREAD], ag_sem.at[u, q], device)

    def wait_spread(u, q):
        def wait(count):
            ref = block(peer(q), u, h).at[pl.ds(0, count)]
            send(ref, ref, sent.at[SPREAD], ag_sem.at[u, q], (g, partner)).wait_recv()

        if owners > 1:
            pl.when(owns)(functools.partial(wait, owners - 1))
        pl.when(jnp.logical_not(owns))(functools.partial(wait, owners))

    def by_piece(k, o, source):
        if k:
            return True
        source_twice = source + groups < rounds
        if o == 1:
            return jnp.logical_not(source_twice)
        return source_twice if o == 3 else False

    def whole(k, o, source):
        piece = by_piece(k, o, source)
        return not piece if isinstance(piece, bool) else jnp.logical_not(piece)

    def only_if(condition, f):
        if condition is True:
            f()
        elif condition is not False:
            pl.when(condition)(f)

    def across(u, o, origin=None):
        ref = block(g if origin is None else origin, u, h)
        return send(ref, ref, sent.at[ACROSS], grp_sem.at[u, o], (peer(o), d))

    def across_piece(u, o, origin=None):
        ref = block(g if origin is None else origin, u, h).at[w]
        return send(ref, ref, sent.at[ACROSS], grp_sem.at[u, o], (peer(o), d))

    def forward(u, o):
        ref = block(peer(o), u, h)
        recv_sem = fwd_sem.at[u // subs * groups + o]
        return send(ref, ref, sent.at[FORWARD], recv_sem, (g, partner))

    def wait_forward(k, o):
        with jax.named_scope("waitfwd"):
            ref = cent.at[peer(o) + groups * k, 1 - h]
            at = k * groups + o
            send(ref, ref, sent.at[FORWARD], fwd_sem.at[at], (g, partner)).wait_recv()

    def if_held(k, o, f):
        if groups * (k + 1) <= rounds:
            f()
        else:
            pl.when(peer(o) + groups * k < rounds)(f)

    def pair_sum(u):
        with jax.named_scope("pairsum"):
            to_partner(u).wait_recv()
            both = own_half[u] + pin[u]
            half[u] = both.reshape(half.shape[1:])

    def add_pair(u):
        if_held(u // subs, 0, functools.partial(pair_sum, u))

    def scatter_unit(u):
        if_held(u // subs, 0, lambda: scatter_all(u))

    def gather_out(u):
        def f():
            gather(u // subs, u % subs, 1 - h, out_half)
            if u == 0:
                with jax.named_scope("barrier"):
                    pl.semaphore_wait(barrier, devs - 1 + groups - 1)
            to_partner(u).start()

        if_held(u // subs, 0, f)

    def gather_own(u):
        if_held(u // subs, 0, lambda: gather(u // subs, u % subs, h, own_half))

    ones_row = jnp.ones((8, width), jnp.bfloat16)

    def row_norms(first, last):
        with jax.named_scope("rownorm"):
            for j in range(first, last):
                at = pl.ds(j * TILE, TILE)
                square = jnp.square(ef[0, at, :]) + jnp.square(ef[1, at, :])
                high = square.astype(jnp.bfloat16)
                low = (square - high.astype(jnp.float32)).astype(jnp.bfloat16)
                both = jnp.concatenate([high, low], axis=1)
                total = lax.dot_general(ones_row, both, NT, preferred_element_type=jnp.float32)
                for q in range(TILE // 128):
                    rn[pl.ds(j * (TILE // 128) + q, 1), :] = total[0:1, q * 128 : (q + 1) * 128]

    def reduce_chips(u):
        def f():
            with jax.named_scope("reduce%d" % u):
                wait_scatter(u)
                total = half[u, w]
                for slot in range(1, chips):
                    total += zin[u, slot]
                block(g, u, h)[w] = total
                for o in range(1, groups):
                    only_if(by_piece(u // subs, o, g), lambda: across_piece(u, o).start())
                for o in range(1, chips):
                    spread(u, o, 0).start()

        if_held(u // subs, 0, lambda: pl.when(owns)(f))

    def pass_piece(u, q):
        def f():
            with jax.named_scope("piece%d_%d" % (u, q)):
                across_piece(u, q, peer(q)).wait_recv()
                for o in range(1, chips):
                    spread(u, o, q).start()

        piece = by_piece(u // subs, q, peer(q))
        if_held(u // subs, q, lambda: only_if(piece, lambda: pl.when(owns)(f)))

    def share(u, q=0):
        def f():
            with jax.named_scope("share%d_%d" % (u, q)):
                k = u // subs
                if q:
                    only_if(by_piece(k, q, peer(q)), lambda: wait_spread(u, q))
                    only_if(whole(k, q, peer(q)), lambda: across(u, q, peer(q)).wait_recv())
                else:
                    wait_spread(u, 0)
                forward(u, q).start()
                if u < subs and q == 0:
                    pl.when(twice)(lambda: across(u, 1).start())
                    pl.when(once)(lambda: across(u, 2).start())

        if_held(u // subs, q, f)

    steps = rows // TILE
    first_units = range(subs)
    late_units = range(subs, slots * subs)

    def start_units(units, scatter_now):
        gather_out(units[0])
        gather_own(units[0])
        for before, u in zip(units, units[1:]):
            gather_out(u)
            add_pair(before)
            if scatter_now:
                scatter_unit(before)
            gather_own(u)
        add_pair(units[-1])
        if scatter_now:
            scatter_unit(units[-1])

    start_units(first_units, True)
    if slots > 1:
        start_units(late_units, False)
    for u in first_units:
        reduce_chips(u)
    row_norms(0, steps // 2)
    for u in late_units[:1]:
        scatter_unit(u)
    row_norms(steps // 2, steps)
    for q in range(1, groups):
        for u in first_units:
            pass_piece(u, q)
    for u in first_units:
        share(u)
        if u == 0:
            for v in late_units[1:]:
                scatter_unit(v)

    def compute(r, read, count):
        centers = read()
        values = centers.astype(jnp.float32)
        norms = jnp.sum(values * values, axis=1, keepdims=True)
        snb[0:count, :] = jnp.broadcast_to(0.5 * norms, (count, 128))
        for j in range(rows // TILE):
            products = lax.dot_general(
                read(), e[pl.ds(j * TILE, TILE), :], NT, preferred_element_type=jnp.float32
            )
            for q in range(TILE // 128):
                score = products[:, q * 128 : (q + 1) * 128] - snb[0:count, :]
                best = jnp.max(score, axis=0, keepdims=True)
                at = pl.ds(j * (TILE // 128) + q, 1)
                near[r, at, :] = jnp.maximum(near[r, at, :], best)

    def lag(u_list, q):
        for u in u_list:
            share(u, q)

    def pieces_in(q):
        for u in late_units:
            pass_piece(u, q)

    def late_pieces_out():
        for u in late_units[:1]:
            reduce_chips(u)
        for u in first_units:
            across(u, 2).start()

    def rest_out():
        for u in late_units[1:]:
            reduce_chips(u)

    def diagonal_out():
        for u in first_units:
            across(u, 3).start()

    HALF, REST, FULL = range(3)
    two_kinds = [HALF, REST, HALF, REST, HALF, REST, FULL, FULL, None, FULL]
    one_kinds = [HALF, REST, HALF, REST, HALF, REST, FULL, HALF, REST, FULL]
    two = [
        (0, 0, []),
        (0, 0, [late_pieces_out]),
        (0, 2, [lambda: lag(first_units, 2), rest_out]),
        (0, 2, []),
        (0, 1, [lambda: lag(first_units, 1), lambda: pieces_in(1)]),
        (0, 1, [lambda: lag(late_units, 0)]),
        (1, 0, [lambda: lag(first_units, 3)]),
        (0, 3, [lambda: lag(late_units, 1)]),
        None,
        (1, 1, []),
    ]
    one = [
        (0, 0, []),
        (0, 0, []),
        (0, 1, [lambda: lag(first_units, 1), diagonal_out]),
        (0, 1, []),
        (0, 3, [lambda: lag(first_units, 3), lambda: pieces_in(2)]),
        (0, 3, [lambda: lag(first_units, 2), lambda: pieces_in(3)]),
        (0, 2, []),
        (1, 2, [lambda: lag(late_units, 2)]),
        (1, 2, [lambda: lag(late_units, 3)]),
        (1, 3, []),
    ]

    def prepare(kind, k, o, actions):
        for action in actions:
            action()
        if kind != HALF:
            wait_forward(k, o)

    def round_of(line):
        return peer(line[1]) + groups * line[0]

    def run(kind, r):
        if kind == FULL:
            with jax.named_scope("compute"):
                compute(r, lambda: cent[r].reshape(seeds, width), seeds)
        else:
            which = h if kind == HALF else 1 - h
            with jax.named_scope("half"):
                compute(r, lambda: cent[r, which].reshape(seeds // 2, width), seeds // 2)

    def step(kind, line):
        prepare(kind, *line)
        run(kind, round_of(line))

    for kind_two, kind_one, line_two, line_one in zip(two_kinds, one_kinds, two, one):
        if kind_two == kind_one:
            pl.when(twice)(functools.partial(prepare, kind_two, *line_two))
            pl.when(once)(functools.partial(prepare, kind_one, *line_one))
            run(kind_two, jnp.where(twice, round_of(line_two), round_of(line_one)))
        else:
            if line_two is not None:
                pl.when(twice)(functools.partial(step, kind_two, line_two))
            pl.when(once)(functools.partial(step, kind_one, line_one))

    with jax.named_scope("final"):
        load_prior.wait()
        current = prior[...]
        norms = rn[...]
        sums = []
        for r in range(rounds):
            gap = jnp.maximum(norms - 2.0 * near[r], 0.0) * (1.0 / width)
            current = jnp.minimum(current, gap)
            sums.append(jnp.sum(current, axis=0, keepdims=True))
        if rounds < 8:
            sums.append(jnp.zeros((8 - rounds, 128), jnp.float32))
        part[...] = jnp.concatenate(sums, axis=0)
        dist[...] = current

    def send_part(o):
        return send(part, parts.at[o], sent.at[MEAN], mean_sem, (g, (d + o) % devs))

    for o in range(1, devs):
        send_part(o).start()

    piece = half_rows // owners

    def cut_up(k, o, source_twice):
        return k > 0 or (not source_twice if o == 1 else source_twice and o == 3)

    def drain(is_two, is_owner):
        held = range(2 if is_two else 1)
        half_unit, own_part = subs * half_rows, subs * piece
        wait_sent(FORWARD, rounds * half_unit)
        wait_sent(PAIR, len(held) * half_unit)
        wait_sent(SCATTER, len(held) * own_part * (owners - 1 if is_owner else owners))
        crossed, spreads = 0, 0
        for k in range(2):
            for o in range(groups):
                source_two = is_two if o < 2 else not is_two
                if k in held and o:
                    in_pieces = cut_up(k, o, is_two)
                    crossed += (own_part if is_owner else 0) if in_pieces else half_unit
                if (k == 0 or source_two) and (o == 0 or cut_up(k, o, source_two)):
                    spreads += own_part * (chips - 1)
        wait_sent(ACROSS, crossed)
        wait_sent(SPREAD, spreads if is_owner else 0)

    with jax.named_scope("drain"):
        for is_two in (True, False):
            for is_owner in (True, False):
                mine = (twice if is_two else once) & (owns if is_owner else jnp.logical_not(owns))
                pl.when(mine)(functools.partial(drain, is_two, is_owner))

    with jax.named_scope("means"):
        total = part[...]
        every = parts.at[pl.ds(1, devs - 1)]
        means_in = send(every, every, sent.at[MEAN], mean_sem, (g, partner))
        means_in.wait_recv()
        for o in range(1, devs):
            total += parts[o]
        column = jnp.sum(total, axis=1, keepdims=True) / float(rows * devs)
        at_row = lax.broadcasted_iota(jnp.int32, (8, 128), 0)
        at_lane = lax.broadcasted_iota(jnp.int32, (8, 128), 1)
        line = jnp.sum(jnp.where(at_row == at_lane, column, 0.0), axis=0, keepdims=True)
        means[...] = jnp.broadcast_to(line, (8, 128))

    means_in.wait_send()


def emit(dist_in, means_in, dist, means):
    dist[...] = dist_in[...]
    means[...] = means_in[0:1, 0 : means.shape[1]]


def body(embeddings, prior_dist, seed_ids):
    rows, width = embeddings.shape
    rounds, seeds = seed_ids.shape
    groups, devs = lax.axis_size("grp"), lax.axis_size("dev")
    chips = devs // 2
    slots = (rounds + groups - 1) // groups
    subs = 2 if seeds // 4 // (chips // 2) >= 16 else 1
    units = slots * subs
    half_rows = seeds // subs // 2
    owners, others = chips // 2, chips - chips // 2
    piece = half_rows // owners
    bf16, f32 = jnp.bfloat16, jnp.float32
    vmem = pl.BlockSpec(memory_space=pltpu.VMEM)
    hbm = pl.BlockSpec(memory_space=pltpu.HBM)
    dist, means = pl.pallas_call(
        functools.partial(kernel, (groups, devs, rounds, seeds, rows, width, subs)),
        out_shape=(pltpu.VMEM((rows // 128, 128), f32), pltpu.VMEM((8, 128), f32)),
        in_specs=[hbm, hbm, hbm],
        out_specs=(vmem, vmem),
        scratch_shapes=[
            pltpu.SMEM((rounds, seeds), jnp.int32),
            pltpu.VMEM((rows // 128, 128), f32),
            pltpu.VMEM((rows, width), bf16),
            pltpu.VMEM((2, rows + 8, width // 2), f32),
            pltpu.VMEM((2, half_rows, width // 2), f32),
            pltpu.VMEM((units, half_rows, width), bf16),
            pltpu.VMEM((units, half_rows, width), bf16),
            pltpu.VMEM((units, half_rows, width), bf16),
            pltpu.VMEM((units, owners, piece, width), bf16),
            pltpu.VMEM((units, owners + others, piece, width), bf16),
            pltpu.VMEM((rounds, 2, subs, owners, piece, width), bf16),
            pltpu.VMEM((seeds, 128), f32),
            pltpu.VMEM((rounds, rows // 128, 128), f32),
            pltpu.VMEM((rows // 128, 128), f32),
            pltpu.VMEM((8, 128), f32),
            pltpu.VMEM((devs, 8, 128), f32),
            pltpu.SemaphoreType.DMA,
            pltpu.SemaphoreType.DMA,
            pltpu.SemaphoreType.DMA((LOAD_CHUNKS,)),
            pltpu.SemaphoreType.DMA((6,)),
            pltpu.SemaphoreType.DMA((units,)),
            pltpu.SemaphoreType.DMA((units,)),
            pltpu.SemaphoreType.DMA((units, groups)),
            pltpu.SemaphoreType.DMA((units, groups)),
            pltpu.SemaphoreType.DMA((slots * groups,)),
            pltpu.SemaphoreType.DMA,
        ],
        compiler_params=pltpu.CompilerParams(
            collective_id=0, has_side_effects=True, vmem_limit_bytes=56 * 1024 * 1024
        ),
        name="seed_rounds",
    )(seed_ids, prior_dist.reshape(rows // 128, 128), embeddings)
    dist, means = pl.pallas_call(
        emit,
        out_shape=(
            jax.ShapeDtypeStruct((rows // 128, 128), f32),
            jax.ShapeDtypeStruct((1, rounds), f32),
        ),
        in_specs=[vmem, vmem],
        out_specs=(vmem, vmem),
        compiler_params=pltpu.CompilerParams(vmem_limit_bytes=1024 * 1024),
        name="emit",
    )(dist, means)
    return dist.reshape(rows), means.reshape(rounds, 1)


def solution(mesh):
    placed = (P(("grp", "dev"), None), P(("grp", "dev")), P())
    return jax.shard_map(
        body,
        mesh=mesh,
        in_specs=placed,
        out_specs=(P(("grp", "dev")), P(None, "grp")),
        check_vma=False,
    )
```
